32 devices in a mesh: gx: 2 (over x), gy: 4 (over y, core), gz: 4 (over z).
Axes of the slice: x: 2, y: 2, z: 4, core: 2. Of those that a mesh axis runs over, the one named last changes fastest.
Arguments:
- metric_pert: float32 [6, 32, 64, 512], P(None, 'gx', 'gy', 'gz'), may hold values from -1.8 to 1.8
- curvature: float32 [6, 32, 64, 512], P(None, 'gx', 'gy', 'gz'), may hold values from -6 to 6
- interp_weights: bfloat16 [2, 4, 32, 64, 4096], P('gx', 'gy', 'gz'), may hold values from -0.09375 to 0.09375
- point_ids: int32 [2, 4, 32, 64], P('gx', 'gy', 'gz'), may hold values from 0 to 6144, as said below
- theta: float32 [6144], replicated, may hold values from 0.05 to 3.09
- phi: float32 [6144], replicated, may hold values from -3.140625 to 3.140625
Outputs:
- psi4_field: bfloat16 [2, 32, 64, 512], P(None, 'gx', 'gy', 'gz')
- modes: float32 [3, 2, 77], replicated
The draws below stay inside these ranges and needn't reach their ends.
Inputs may be any that keep to these rules, and one draw needn't show every extreme that they name: `point_ids`: the grid is a window of the extraction region that the spheres cross. A live entry names a sphere point; the value 6144 marks an empty slot, and each list holds its live entries first. The points of sphere s lie in the 9 consecutive block layers along the third dimension that begin at layer s * 10; each point belongs to one column (bx, by) and is listed in exactly two blocks of that column that are adjacent along the third dimension. Some block's list is full, every listing block holds at least 32 live entries, and blocks outside these layers list no point.
All inputs are finite; a program needn't handle non-finite values.
Results may differ from the reference program's by a relative error of at most 0.0032.
Values sent between devices are 32-bit elements; how exact they have to be, the bound alone decides.
No kernel may reach another device: no remote copies, remote signals or barrier semaphores. Data moves between devices by JAX's collectives and lax.ppermute only.
A program may use at most 64 MiB of HBM per device.

```python
import math
import jax
import jax.numpy as jnp
import numpy as np
from jax import lax

BLK = 16
PB = 64
PTS = 2048
SPHERES = 3
LMAX = 8
NX = 32
NY = 64
NZ = 512
NBX = 2
NBY = 4
NBZ = 32
COL_PTS = 256
RUNS = 8
TOTAL_PTS = 6144


def draw_point_ids(key, part):
    columns = NBX * NBY
    half = PB // 2
    keys = jax.random.split(key, SPHERES * columns)
    orders = jax.vmap(lambda subkey: jax.random.permutation(subkey, COL_PTS))(keys).reshape(SPHERES, columns, COL_PTS)
    base = (jnp.arange(SPHERES) * PTS)[:, None, None] + (jnp.arange(columns) * COL_PTS)[None, :, None]
    listed = (base + orders).astype(jnp.int32).reshape(SPHERES, columns, RUNS, half)
    layer = jnp.arange(RUNS + 1)
    earlier = listed[:, :, jnp.maximum(layer - 1, 0)]
    current = listed[:, :, jnp.minimum(layer, RUNS - 1)]
    live = ((layer >= 1) & (layer <= RUNS - 1))[None, None, :, None]
    current = jnp.where(live, current, TOTAL_PTS)
    lists = jnp.concatenate([earlier, current], 3).astype(jnp.int32)
    result = jnp.full((columns, NBZ, PB), TOTAL_PTS, jnp.int32)
    spacing = NBZ // SPHERES
    for sphere in range(SPHERES):
        result = result.at[:, sphere * spacing:sphere * spacing + RUNS + 1].set(lists[sphere])
    return result.reshape(NBX, NBY, NBZ, PB).astype(jnp.int32)


def levels(stream_key, shape, pieces, low, high):
    factor_of, own = 1.0, jax.random.fold_in(stream_key, 6)
    for dim, shards_of in pieces:
        heights = jnp.exp(jax.random.uniform(jax.random.fold_in(own, dim), (shards_of,), jnp.float32, low / len(pieces), high / len(pieces)))
        factor_of = factor_of * jnp.repeat(heights, shape[dim] // shards_of).reshape([-1 if axis == dim else 1 for axis in range(len(shape))])
    return factor_of


def normal_values(own_key, shape, scale, reach, pieces=(), held_as=jnp.bfloat16):
    values = scale * jax.random.normal(own_key, shape, jnp.float32)
    if pieces:
        values = values * levels(own_key, shape, pieces, -0.22, 0.18)
    return jnp.clip(values, -reach, reach).astype(held_as)


def setup_inputs(seed: int = 0) -> dict:
    key_list = jax.random.split(jax.random.key(seed), 7)
    return {
        "metric_pert": normal_values(key_list[0], (6, NX, NY, NZ), 0.3, 1.8, ((1, 2), (2, 4), (3, 4)), jnp.float32),
        "curvature": normal_values(key_list[1], (6, NX, NY, NZ), 1.0, 6.0, ((1, 2), (2, 4), (3, 4)), jnp.float32),
        "interp_weights": normal_values(key_list[2], (NBX, NBY, NBZ, PB, BLK * BLK * BLK), (BLK * BLK * BLK) ** -0.5, 0.09375, ((0, 2), (1, 4), (2, 4))),
        "point_ids": draw_point_ids(jax.random.fold_in(key_list[6], 71), 0),
        "theta": jnp.clip(jax.random.uniform(key_list[4], (TOTAL_PTS,), jnp.float32, 0.05, 3.09), 0.05, 3.09),
        "phi": jnp.clip(jax.random.uniform(key_list[5], (TOTAL_PTS,), jnp.float32, -3.140625, 3.140625), -3.140625, 3.140625),
    }


PAIRS = [[0, 1, 2], [1, 3, 4], [2, 4, 5]]

def build_table(degree_max):
    width = 2 * degree_max + 1
    columns = []
    orders = []
    for degree in range(2, degree_max + 1):
        for order in range(-degree, degree + 1):
            column = np.zeros(width * width)
            lead = (-1.0) ** order * math.sqrt(math.factorial(degree + order) * math.factorial(degree - order) * (2 * degree + 1) / (4.0 * math.pi * math.factorial(degree - 2) * math.factorial(degree + 2)))
            for step in range(0, degree + 3):
                lower = step - 2 - order
                if lower >= 0 and lower <= degree - 2:
                    value = lead * math.comb(degree + 2, step) * math.comb(degree - 2, lower) * (-1.0) ** (degree - step + 2)
                    expo = 2 * step - 2 - order
                    column[expo * width + (2 * degree - expo)] += value
            columns.append(column)
            orders.append(order)
    return (np.stack(columns, 1), np.array(orders))

def project(sphere_vals, theta, phi, member):
    table, orders = build_table(LMAX)
    width = 2 * LMAX + 1
    cosine = jnp.cos(theta * 0.5)
    sine = jnp.sin(theta * 0.5)
    cos_pow = jnp.stack([cosine ** power for power in range(width)], 1)
    sin_pow = jnp.stack([sine ** power for power in range(width)], 1)
    grid_pow = (cos_pow[:, :, None] * sin_pow[:, None, :]).reshape(theta.shape[0], width * width)
    amplitude = jnp.dot(grid_pow, jnp.asarray(table, jnp.float32), precision=lax.Precision.HIGHEST)
    angle_m = phi[:, None] * jnp.asarray(orders, jnp.float32)[None, :]
    y_real = amplitude * jnp.cos(angle_m)
    y_imag = amplitude * jnp.sin(angle_m)
    left_re = member * sphere_vals[0][None, :]
    left_im = member * sphere_vals[1][None, :]
    highest = lax.Precision.HIGHEST
    real = jnp.dot(left_re, y_real, precision=highest) + jnp.dot(left_im, y_imag, precision=highest)
    imag = jnp.dot(left_im, y_real, precision=highest) - jnp.dot(left_re, y_imag, precision=highest)
    return jnp.stack([real, imag], 1) * (4.0 * math.pi / PTS)

def weyl_scalar(padded, x_coord, y_coord, z_coord):
    extent = [x_coord.shape[0], y_coord.shape[0], z_coord.shape[0]]

    def moved(comp, axis, offset):
        index = [slice(2, 2 + count) for count in extent]
        index[axis] = slice(2 + offset, 2 + offset + extent[axis])
        return padded[comp][tuple(index)]

    def first(comp, axis):
        return (moved(comp, axis, -2) - 8.0 * moved(comp, axis, -1) + 8.0 * moved(comp, axis, 1) - moved(comp, axis, 2)) / 12.0

    def second(comp, axis):
        return (-moved(comp, axis, -2) + 16.0 * moved(comp, axis, -1) - 30.0 * moved(comp, axis, 0) + 16.0 * moved(comp, axis, 1) - moved(comp, axis, 2)) / 12.0
    kval = [moved(6 + comp, 0, 0) for comp in range(6)]
    trace = kval[0] + kval[3] + kval[5]
    electric = {}
    for row in range(3):
        for col in range(row, 3):
            comp = PAIRS[row][col]
            laplace = second(comp, 0) + second(comp, 1) + second(comp, 2)
            square = kval[PAIRS[row][0]] * kval[PAIRS[0][col]] + kval[PAIRS[row][1]] * kval[PAIRS[1][col]] + kval[PAIRS[row][2]] * kval[PAIRS[2][col]]
            value = -0.5 * laplace + trace * kval[comp] - square
            electric[row, col] = value
            electric[col, row] = value
    deriv = [[first(6 + comp, axis) for comp in range(6)] for axis in range(3)]
    curl = {}
    for row in range(3):
        one = (row + 1) % 3
        two = (row + 2) % 3
        for col in range(3):
            curl[row, col] = deriv[one][PAIRS[two][col]] - deriv[two][PAIRS[one][col]]
    x_full = x_coord[:, None, None]
    y_full = y_coord[None, :, None]
    z_full = z_coord[None, None, :]
    radial_xy = jnp.sqrt(x_full * x_full + y_full * y_full)
    radius = jnp.sqrt(radial_xy * radial_xy + z_full * z_full)
    cos_phi = x_full / radial_xy
    sin_phi = y_full / radial_xy
    cos_theta = z_full / radius
    sin_theta = radial_xy / radius
    e_theta = [cos_theta * cos_phi, cos_theta * sin_phi, -sin_theta]
    e_phi = [-sin_phi, cos_phi, 0.0 * cos_phi]
    real = 0.0
    imag = 0.0
    for row in range(3):
        for col in range(3):
            magnetic = 0.5 * (curl[row, col] + curl[col, row])
            plus = 0.5 * (e_theta[row] * e_theta[col] - e_phi[row] * e_phi[col])
            cross = 0.5 * (e_theta[row] * e_phi[col] + e_phi[row] * e_theta[col])
            real = real + electric[row, col] * plus - magnetic * cross
            imag = imag - electric[row, col] * cross - magnetic * plus
    return jnp.stack([real, imag]).astype(jnp.float32)

def reference(metric_pert, curvature, interp_weights, point_ids, theta, phi):
    fields = jnp.concatenate([metric_pert, curvature], 0)
    padded = jnp.pad(fields, ((0, 0), (2, 2), (2, 2), (2, 2)))
    size_x, size_y, size_z = (metric_pert.shape[1], metric_pert.shape[2], metric_pert.shape[3])
    y_coord = jnp.arange(size_y).astype(jnp.float32) + 0.5 - size_y / 2.0
    z_coord = jnp.arange(size_z).astype(jnp.float32) + 0.5 - size_z / 2.0
    slabs = []
    dense = jnp.zeros((TOTAL_PTS + 1, 2), jnp.float32)
    for block_x in range(NBX):
        slab = padded[:, block_x * BLK:block_x * BLK + BLK + 4]
        x_coord = (jnp.arange(BLK) + block_x * BLK).astype(jnp.float32) + 0.5 - size_x / 2.0
        psi_slab = weyl_scalar(slab, x_coord, y_coord, z_coord).astype(jnp.bfloat16)
        slabs.append(psi_slab)
        blocks = psi_slab.reshape(2, BLK, NBY, BLK, NBZ, BLK).transpose(2, 4, 0, 1, 3, 5).reshape(NBY, NBZ, 2, BLK * BLK * BLK)
        partial_value = jnp.einsum('yzcn,yzpn->yzpc', blocks.astype(jnp.float32), interp_weights[block_x].astype(jnp.float32), precision=lax.Precision.HIGHEST)
        dense = dense + jax.ops.segment_sum(partial_value.reshape(-1, 2), point_ids[block_x].reshape(-1), num_segments=TOTAL_PTS + 1)
    psi4_field = jnp.concatenate(slabs, 1)
    sphere_vals = dense[:TOTAL_PTS].T
    point_index = jnp.arange(TOTAL_PTS)
    member = (point_index[None, :] // PTS == jnp.arange(SPHERES)[:, None]).astype(jnp.float32)
    modes = project(sphere_vals, theta, phi, member)
    return (psi4_field, modes)
```

```python
import functools
import math

import jax
import jax.numpy as jnp
import numpy as np
from jax import lax
from jax.experimental import pallas as pl
from jax.experimental.pallas import tpu as pltpu
from jax.sharding import PartitionSpec as P

BLK = 16
PTS = 2048
SPHERES = 3
LMAX = 8
AXES = ("gx", "gy", "gz")
MODES = (LMAX + 1) ** 2 - 4
ROWS = 24
NEAR = 1.0 / 3.0
FAR = 1.0 / 24.0
XX, XY, XZ, YY, YZ, ZZ = range(6)
VMEM = pltpu.VMEM
LIMIT = 24 * 1024 * 1024


def recurrence():
    table = np.zeros((ROWS, 128), np.float32)
    norm = lambda degree: math.sqrt((2 * degree + 1) / (4.0 * math.pi))
    for order in range(-LMAX, LMAX + 1):
        low = max(2, abs(order))
        row = order + LMAX
        gap = lambda degree: math.sqrt((degree**2 - order**2) * (degree**2 - 4))
        for degree in range(low, LMAX):
            base = 3 * (degree - 2)
            lift = degree * gap(degree + 1)
            scale = norm(degree + 1) / norm(degree) * (2 * degree + 1) / lift
            table[row, base] = scale * degree * (degree + 1)
            table[row, base + 1] = -scale * 2 * order
            if degree > low:
                table[row, base + 2] = norm(degree + 1) / norm(degree - 1) * (degree + 1) * gap(degree) / lift
        step = min(max(order, -2), 2) + 2 if low == 2 else (low + 2 if order > 0 else 0)
        lower = step - 2 - order
        lead = (-1.0) ** order * math.sqrt(
            math.factorial(low + order)
            * math.factorial(low - order)
            * (2 * low + 1)
            / (4.0 * math.pi * math.factorial(low - 2) * math.factorial(low + 2))
        )
        table[row, 127] = lead * math.comb(low + 2, step) * math.comb(low - 2, lower) * (-1.0) ** (low - step + 2)
    return table


def frame(x, y, z):
    rho2 = x * x + y * y
    inv_rho = lax.rsqrt(rho2)
    inv_r = lax.rsqrt(rho2 + z * z)
    cos_p = x * inv_rho
    sin_p = y * inv_rho
    cos_t = z * inv_r
    sin_t = rho2 * inv_rho * inv_r
    cc = cos_p * cos_p
    ss = sin_p * sin_p
    tt = cos_t * cos_t
    cs = cos_p * sin_p
    st = sin_t * cos_t
    twice_p = (tt * cc - ss, cs * (tt + 1.0), -(st * cos_p), tt * ss - cc, -(st * sin_p), sin_t * sin_t)
    q_diag = cos_t * cs
    twice_q = (cos_t * (cc - ss), sin_t * sin_p, -(sin_t * cos_p))
    return twice_p, q_diag, twice_q


def total(terms):
    terms = [term for term in terms if term is not None]
    return functools.reduce(lambda one, two: one + two, terms)


def times(one, two):
    return None if one is None or two is None else one * two


def minus(one, two):
    if two is None:
        return one
    return -two if one is None else one - two


def contract(geometry, electric, magnetic):
    twice_p, q_diag, twice_q = geometry
    e, b = electric, magnetic
    half = total([times(twice_p[i], e[i]) for i in (XX, YY, ZZ)]) * 0.5
    real_e = half + total([times(twice_p[i], e[i]) for i in (XY, XZ, YZ)])
    off = (XY, XZ, YZ)
    imag_e = q_diag * (e[YY] - e[XX]) + total([twice_q[n] * e[i] for n, i in enumerate(off)])
    real_b = total([times(2.0 * q_diag, minus(b[YY], b[XX]))] + [times(twice_q[n], b[i]) for n, i in enumerate(off)])
    imag_b = total([times(twice_p[i], b[i]) for i in range(6)])
    return real_e - real_b, -(imag_e + imag_b)


def curl_part(axis, d):
    yz, xz, xy, diff = d
    if axis == 0:
        return [None, -xz, xy, -yz, diff, yz]
    if axis == 1:
        return [xz, yz, diff, None, -xy, -xz]
    return [-xy, diff, -yz, xy, xz, None]


DIFFS = ((YY, ZZ), (ZZ, XX), (XX, YY))


def iota(shape, dim):
    return lax.broadcasted_iota(jnp.int32, shape, dim)


def origin(axis, cells):
    place = lax.axis_index(axis)
    count = lax.axis_size(axis)
    return (place * cells).astype(jnp.float32) + (0.5 - count * cells / 2.0), place


def face_part(axis, near, far, sign, geometry):
    h_near, k_near = near if near is not None else (None, None)
    h_far, k_far = far
    if near is None:
        e = [h * FAR for h in h_far]
        d = [k * (-FAR * sign) for k in k_far]
    else:
        e = [f * FAR - n * (2.0 / 3.0) for n, f in zip(h_near, h_far)]
        d = [(n * NEAR - f * FAR) * sign for n, f in zip(k_near, k_far)]
    return contract(geometry, e, curl_part(axis, d))


def pick_k(axis, load):
    one, two = DIFFS[axis]
    return [load(6 + YZ), load(6 + XZ), load(6 + XY), load(6 + one) - load(6 + two)]


def faces_kernel(slots, metric, curvature, *refs):
    nx = slots[0]
    ny = slots[1]
    x_out = refs[:nx]
    y_out = refs[nx : nx + ny]
    z_out, z_fix, fields, sems = refs[nx + ny :]
    copies = []
    for comp in range(6):
        for base, source in ((0, metric), (6, curvature)):
            copies.append(
                pltpu.make_async_copy(
                    source.at[comp],
                    fields.at[base + comp, pl.ds(2, BLK), pl.ds(8, BLK), :],
                    sems.at[base + comp],
                )
            )
    for copy in copies:
        copy.start()
    blank = jnp.zeros((12, BLK, 8, 128), jnp.float32)
    fields[:, pl.ds(2, BLK), pl.ds(0, 8), :] = blank
    fields[:, pl.ds(2, BLK), pl.ds(24, 8), :] = blank
    plane = jnp.zeros((12, 2, BLK, 128), jnp.float32)
    fields[:, pl.ds(0, 2), pl.ds(8, BLK), :] = plane
    fields[:, pl.ds(BLK + 2, 2), pl.ds(8, BLK), :] = plane
    for copy in copies:
        copy.wait()
    x0, ix = origin("gx", BLK)
    y0, iy = origin("gy", BLK)
    z0, iz = origin("gz", 128)
    slab = (BLK, 128)
    rows = iota(slab, 0).astype(jnp.float32)
    lanes = iota(slab, 1).astype(jnp.float32)
    z = lanes + z0
    for slot in range(nx):
        high = (ix % 2) == slot
        near_at = jnp.where(high, BLK + 1, 2)
        far_at = jnp.where(high, BLK, 3)
        sign = jnp.where(high, -1.0, 1.0)
        near = [fields[c, near_at, pl.ds(8, BLK), :] for c in range(6)]
        far = [fields[c, far_at, pl.ds(8, BLK), :] for c in range(6)]
        k_near = pick_k(0, lambda c: fields[c, near_at, pl.ds(8, BLK), :])
        k_far = pick_k(0, lambda c: fields[c, far_at, pl.ds(8, BLK), :])
        y = rows + y0
        for layer in range(2):
            x = jnp.where(high, x0 + (BLK + layer), x0 - (1 + layer))
            geometry = frame(x, y, z)
            if layer == 0:
                real, imag = face_part(0, (near, k_near), (far, k_far), sign, geometry)
            else:
                real, imag = face_part(0, None, (near, k_near), sign, geometry)
            x_out[slot][0, layer] = real
            x_out[slot][1, layer] = imag
    for slot in range(ny):
        high = (iy % 2) == slot
        near_at = jnp.where(high, 8 + BLK - 1, 8)
        far_at = jnp.where(high, 8 + BLK - 2, 9)
        sign = jnp.where(high, -1.0, 1.0)

        def line(c, at):
            return fields.reshape(12 * 20 * 32, 128)[pl.ds(c * 640 + 64 + at, BLK, stride=32), :]

        near = [line(c, near_at) for c in range(6)]
        far = [line(c, far_at) for c in range(6)]
        k_near = pick_k(1, lambda c: line(c, near_at))
        k_far = pick_k(1, lambda c: line(c, far_at))
        x = rows + x0
        for layer in range(2):
            y = jnp.where(high, y0 + (BLK + layer), y0 - (1 + layer))
            geometry = frame(x, y, z)
            if layer == 0:
                real, imag = face_part(1, (near, k_near), (far, k_far), sign, geometry)
            else:
                real, imag = face_part(1, None, (near, k_near), sign, geometry)
            y_out[slot][0, layer] = real
            y_out[slot][1, layer] = imag
    lane = iota((8, 128), 1)
    group = lane // 4

    def packed(load):
        out = jnp.zeros((8, 128), jnp.float32)
        for j in range(32):
            value = load(j // 2, j % 2)
            out = jnp.where(group == j, pltpu.roll(value, (2 + 4 * j) % 128, 1), out)
        return out

    def piece(c):
        return lambda x, half: fields[c, 2 + x, pl.ds(8 + 8 * half, 8), :]

    h_all = [packed(piece(c)) for c in range(6)]
    one, two = DIFFS[2]
    k_all = [packed(piece(6 + c)) for c in (YZ, XZ, XY)]
    k_all.append(packed(lambda x, half: piece(6 + one)(x, half) - piece(6 + two)(x, half)))
    q = lane % 4
    upper = q >= 2
    inner = (q == 1) | (q == 2)

    def shifted(value, by):
        return jnp.where(upper, pltpu.roll(value, by, 1), pltpu.roll(value, 128 - by, 1))

    e = [shifted(h, 2) * FAR - jnp.where(inner, shifted(h, 1), 0.0) * (2.0 / 3.0) for h in h_all]
    sign = jnp.where(upper, -1.0, 1.0)
    d = [(jnp.where(inner, shifted(k, 1), 0.0) * NEAR - shifted(k, 2) * FAR) * sign for k in k_all]
    magnetic = curl_part(2, d)
    x = (lane // 8).astype(jnp.float32) + x0
    y = (iota((8, 128), 0) + 8 * (group % 2)).astype(jnp.float32) + y0
    z_here = jnp.where(upper, q - 2, q + 126).astype(jnp.float32) + z0
    z_there = z_here + jnp.where(upper, 128.0, -128.0)
    for out, z_at in ((z_out, z_there), (z_fix, z_here)):
        real, imag = contract(frame(x, y, z_at), e, magnetic)
        out[0] = real
        out[1] = imag


def sin_cos(x):
    x2 = x * x
    sine = 0.0
    cosine = 0.0
    for n in range(6, -1, -1):
        sine = sine * x2 + (-1.0) ** n / math.factorial(2 * n + 1)
    for n in range(7, -1, -1):
        cosine = cosine * x2 + (-1.0) ** n / math.factorial(2 * n)
    return sine * x, cosine


def split3(value):
    one = value.astype(jnp.bfloat16)
    rest = value - one.astype(jnp.float32)
    two = rest.astype(jnp.bfloat16)
    three = (rest - two.astype(jnp.float32)).astype(jnp.bfloat16)
    return one, two, three


def interior_kernel(fields, ids_far, theta_far, phi_far, coefs_far, weights, local, harm, ids, loaded, *scratch):
    lists, theta, phi, coefs, sems = scratch
    small = [
        pltpu.make_async_copy(source, target, sems.at[n])
        for n, (source, target) in enumerate(
            ((ids_far, lists), (theta_far, theta), (phi_far, phi), (coefs_far, coefs))
        )
    ]
    copy = pltpu.make_async_copy(weights, loaded, sems.at[4])
    for each in small:
        each.start()
    copy.start()
    x0, _ = origin("gx", BLK)
    y0, _ = origin("gy", BLK)
    z0, _ = origin("gz", 128)
    slab = (BLK, 128)
    y = iota(slab, 0).astype(jnp.float32) + y0
    z = iota(slab, 1).astype(jnp.float32) + z0

    def plane(i, carry):
        def at(c, dx=0, dy=0):
            return fields[c, i + (2 + dx), pl.ds(8 + dy, BLK), :]

        def roll(value, by):
            return pltpu.roll(value, by % 128, 1)

        geometry = frame(x0 + i.astype(jnp.float32), y, z)
        k = [at(6 + c) for c in range(6)]
        trace = k[XX] + k[YY] + k[ZZ]
        prod = {}

        def mul(a, b):
            key = (min(a, b), max(a, b))
            if key not in prod:
                prod[key] = k[key[0]] * k[key[1]]
            return prod[key]

        pairs = ((XX, XY, XZ), (XY, YY, YZ), (XZ, YZ, ZZ))
        e = []
        for row in range(3):
            for col in range(row, 3):
                c = pairs[row][col]
                h = at(c)
                one = (at(c, -1) + at(c, 1)) + (at(c, 0, -1) + at(c, 0, 1)) + (roll(h, 1) + roll(h, -1))
                two = (at(c, -2) + at(c, 2)) + (at(c, 0, -2) + at(c, 0, 2)) + (roll(h, 2) + roll(h, -2))
                square = total([mul(pairs[row][n], pairs[n][col]) for n in range(3)])
                e.append(two * FAR - one * (2.0 / 3.0) + h * 3.75 + (trace * k[c] - square))

        def slope(m2, m1, p1, p2):
            return (p1 - m1) * NEAR - (p2 - m2) * FAR

        steps = (-2, -1, 1, 2)
        along_x = [pick_k(0, lambda c, s=s: at(c, s)) for s in steps]
        dx = [slope(*[along_x[n][f] for n in range(4)]) for f in range(4)]
        along_y = [pick_k(1, lambda c, s=s: at(c, 0, s)) for s in steps]
        dy = [slope(*[along_y[n][f] for n in range(4)]) for f in range(4)]
        here = [k[YZ], k[XZ], k[XY], k[XX] - k[YY]]
        dz = [slope(*[roll(f, -s) for s in steps]) for f in here]
        parts = [curl_part(axis, d) for axis, d in enumerate((dx, dy, dz))]
        magnetic = [total([part[c] for part in parts]) for c in range(6)]
        real, imag = contract(geometry, e, magnetic)
        local[0, i] = real
        local[1, i] = imag
        return carry

    lax.fori_loop(0, BLK, plane, 0)
    for each in small:
        each.wait()
    count = ids.shape[1]
    id_row = jnp.concatenate([lists[n : n + 1] for n in range(lists.shape[0])], axis=1)
    ids[...] = id_row
    wide = (theta.shape[0], count)
    pick = jnp.where(iota(wide, 0) == id_row // 128, 1.0, 0.0).astype(jnp.bfloat16)
    tables = jnp.concatenate([theta[...], phi[...]], axis=1)
    left = jnp.concatenate(split3(tables), axis=0)
    right = jnp.concatenate([pick] * 3, axis=0)
    found = lax.dot_general(left, right, (((0,), (0,)), ((), ())), preferred_element_type=jnp.float32)
    mine = iota((128, count), 0) == id_row % 128
    half_t = jnp.sum(jnp.where(mine, found[:128], 0.0), axis=0, keepdims=True) * 0.5
    half_p = jnp.sum(jnp.where(mine, found[128:], 0.0), axis=0, keepdims=True) * 0.5
    sines, cosines = sin_cos(jnp.concatenate([half_t, half_p, jnp.zeros((6, count), jnp.float32)], axis=0))
    sin_h, cos_h = sines[0:1], cosines[0:1]
    cos_t = cos_h * cos_h - sin_h * sin_h
    sin_p = 2.0 * sines[1:2] * cosines[1:2]
    cos_p = 1.0 - 2.0 * sines[1:2] * sines[1:2]
    shape = (ROWS, count)
    order = iota(shape, 0) - LMAX
    size = jnp.abs(order)
    lowest = jnp.maximum(size, 2)
    tilt = jnp.clip(order, -2, 2)
    unit_r = jnp.ones(shape, jnp.float32)
    unit_i = jnp.zeros(shape, jnp.float32)
    start = jnp.where(size <= LMAX, coefs[:, 127:128], 0.0)
    step_r, step_i, step_c, step_s = cos_p, sin_p, cos_h, sin_h
    for bit in range(4):
        has = (size >> bit) & 1 == 1
        new_r = unit_r * step_r - unit_i * step_i
        new_i = unit_r * step_i + unit_i * step_r
        unit_r = jnp.where(has, new_r, unit_r)
        unit_i = jnp.where(has, new_i, unit_i)
        start = jnp.where(((lowest + tilt) >> bit) & 1 == 1, start * step_c, start)
        start = jnp.where(((lowest - tilt) >> bit) & 1 == 1, start * step_s, start)
        step_r, step_i = step_r * step_r - step_i * step_i, 2.0 * step_r * step_i
        step_c = step_c * step_c
        step_s = step_s * step_s
    unit_i = jnp.where(order < 0, -unit_i, unit_i)
    before = jnp.zeros(shape, jnp.float32)
    now = jnp.where(lowest == 2, start, 0.0)
    for degree in range(2, LMAX + 1):
        if degree > 2:
            base = 3 * (degree - 3)
            slope = coefs[:, base : base + 1] * cos_t + coefs[:, base + 1 : base + 2]
            after = slope * now - coefs[:, base + 2 : base + 3] * before
            before, now = now, jnp.where(lowest == degree, start, after)
        at = degree * degree - 4
        width = 2 * degree + 1
        low = LMAX - degree
        harm[pl.ds(at, width), pl.ds(0, count)] = (now * unit_r)[low : low + width]
        harm[pl.ds(at, width), pl.ds(count, count)] = (now * unit_i)[low : low + width]
    harm[pl.ds(MODES, 80 - MODES), :] = jnp.zeros((80 - MODES, 2 * count), jnp.float32)
    copy.wait()


def finish_kernel(slots, local, *refs):
    nx, ny, nz = slots
    x_in = refs[:nx]
    y_in = refs[nx : nx + ny]
    z_in = refs[nx + ny : nx + ny + nz]
    z_fix, weights, harm, ids, psi, modes, work, stored, flat, sem = refs[nx + ny + nz :]
    ix = lax.axis_index("gx")
    iy = lax.axis_index("gy")
    iz = lax.axis_index("gz")
    lane = iota((8, 128), 1)
    q = lane % 4
    edge = (lane >= 126) | (lane < 2)
    for part in range(2):
        got = [ref[part] for ref in z_in]
        if nz == 1:
            got = got * 2
        even = (iz % 2) == 0
        plus = jnp.where(even, got[0], got[1])
        less = jnp.where(even, got[1], got[0])
        z_part = jnp.where(q < 2, plus, less)
        if nz == 1:
            z_part = jnp.where((q < 2) == even, got[0], 0.0)
        z_part = z_part - z_fix[part]
        for j in range(32):
            moved = pltpu.roll(z_part, (126 - 4 * j) % 128, 1)
            value = local[part, j // 2, pl.ds(8 * (j % 2), 8), :]
            work[part, pl.ds(8 * j, 8), :] = value + jnp.where(edge, moved, 0.0)
    for part in range(2):
        for slot in range(nx):
            high = (ix % 2) == slot
            for layer in range(2):
                at = jnp.where(high, BLK - 1 - layer, layer) * BLK
                span = pl.ds(pl.multiple_of(at, BLK), BLK)
                work[part, span, :] = work[part, span, :] + x_in[slot][part, layer]
        for slot in range(ny):
            high = (iy % 2) == slot
            for layer in range(2):
                at = jnp.where(high, BLK - 1 - layer, layer)
                span = pl.ds(part * 256 + at, BLK, stride=BLK)
                both = work.reshape(512, 128)
                both[span, :] = both[span, :] + y_in[slot][part, layer]
    row = iota((8, 128), 0)
    source = (lane // BLK + row + 1) % 8
    for part in range(2):
        for x in range(BLK):
            rounded = work[part, pl.ds(BLK * x, BLK), :].astype(jnp.bfloat16)
            stored[part, x] = rounded
            values = rounded.astype(jnp.float32)
            for half in range(2):
                value = values[8 * half : 8 * half + 8]
                value = pltpu.roll(value, 0, 1, stride=BLK, stride_axis=0)
                value = jnp.take_along_axis(value, source, axis=0)
                value = pltpu.roll(value, BLK, 1, stride=BLK, stride_axis=0)
                flat[pl.ds(8 * part, 8), pl.ds((2 * x + half) * 128, 128)] = value
    copy = pltpu.make_async_copy(stored, psi, sem)
    copy.start()
    count = ids.shape[1]
    blocks = flat[...].astype(jnp.bfloat16)
    product = lax.dot_general(
        blocks, weights[...], (((1,), (1,)), ((), ())), preferred_element_type=jnp.float32
    )
    own = iota((8, count), 0) == 7 - iota((8, count), 1) // (count // 8)
    real = jnp.sum(jnp.where(own, product[:8], 0.0), axis=0, keepdims=True)
    imag = jnp.sum(jnp.where(own, product[8:], 0.0), axis=0, keepdims=True)
    row = iota((8, count), 0)
    live = ids[...] // PTS == row // 2
    first = row % 2 == 0
    left = jnp.where(live, jnp.where(first, real, imag), 0.0)
    right = jnp.where(live, jnp.where(first, imag, -real), 0.0)
    sums = lax.dot_general(
        jnp.concatenate([left, right], axis=1),
        harm[...],
        (((1,), (1,)), ((), ())),
        precision=lax.Precision.HIGHEST,
        preferred_element_type=jnp.float32,
    )
    sums = sums * (4.0 * math.pi / PTS)
    sums = jnp.concatenate([sums, jnp.zeros((8, 128 - 80), jnp.float32)], axis=1)
    modes[...] = jnp.broadcast_to(sums[None], modes.shape)
    copy.wait()


def matching(axis, slot):
    perm = []
    for low in range(slot, lax.axis_size(axis) - 1, 2):
        perm += [(low, low + 1), (low + 1, low)]
    return perm


def shards(metric_pert, curvature, interp_weights, point_ids, theta, phi):
    f32 = jnp.float32
    hbm = pl.BlockSpec(memory_space=pltpu.HBM)
    far = lambda value: pltpu.with_memory_space_constraint(value, pltpu.HBM)
    close = lambda value: pltpu.with_memory_space_constraint(value, VMEM)
    vmem = pl.BlockSpec(memory_space=VMEM)
    slots = tuple(min(2, lax.axis_size(axis) - 1) for axis in AXES)
    nx, ny, nz = slots
    count = point_ids.size
    lists = point_ids.shape[2:]
    cells = BLK * BLK * BLK
    face = VMEM((2, 2, BLK, 128), f32)
    edge = VMEM((2, 8, 128), f32)
    params = pltpu.CompilerParams(vmem_limit_bytes=LIMIT)
    first = pl.pallas_call(
        functools.partial(faces_kernel, slots),
        out_shape=[face] * (nx + ny) + [edge, edge, VMEM((12, 20, 32, 128), f32)],
        in_specs=[hbm] * 2,
        out_specs=[vmem] * (nx + ny + 3),
        scratch_shapes=[pltpu.SemaphoreType.DMA((12,))],
        compiler_params=params,
        name="faces",
    )(far(metric_pert), far(curvature))
    x_send, y_send = first[:nx], first[nx : nx + ny]
    z_send, z_fix, fields = first[nx + ny :]
    x_got = [lax.ppermute(x_send[slot], "gx", matching("gx", slot)) for slot in range(nx)]
    y_got = [lax.ppermute(y_send[slot], "gy", matching("gy", slot)) for slot in range(ny)]
    z_got = [lax.ppermute(z_send, "gz", matching("gz", slot)) for slot in range(nz)]
    weights = interp_weights.reshape(count, cells)
    local, harm, ids, loaded = pl.pallas_call(
        interior_kernel,
        out_shape=[VMEM((2, BLK, BLK, 128), f32), VMEM((80, 2 * count), f32), VMEM((1, count), jnp.int32), VMEM((count, cells), jnp.bfloat16)],
        in_specs=[vmem] + [hbm] * 5,
        out_specs=[vmem] * 4,
        scratch_shapes=[
            VMEM(lists, jnp.int32),
            VMEM((theta.size // 128, 128), f32),
            VMEM((theta.size // 128, 128), f32),
            VMEM((ROWS, 128), f32),
            pltpu.SemaphoreType.DMA((5,)),
        ],
        compiler_params=params,
        cost_estimate=pl.CostEstimate(flops=20_000_000, bytes_accessed=8_000_000, transcendentals=0),
        name="interior",
    )(
        close(fields),
        far(point_ids.reshape(lists)),
        far(theta.reshape(-1, 128)),
        far(phi.reshape(-1, 128)),
        far(jnp.asarray(recurrence())),
        far(weights),
    )
    total_devices = math.prod(lax.axis_size(axis) for axis in AXES)
    psi, modes = pl.pallas_call(
        functools.partial(finish_kernel, slots),
        out_shape=[pltpu.HBM((2, BLK, BLK, 128), jnp.bfloat16), VMEM((total_devices, 8, 128), f32)],
        in_specs=[vmem] * (1 + nx + ny + nz + 4),
        out_specs=[hbm, vmem],
        scratch_shapes=[
            VMEM((2, 256, 128), f32),
            VMEM((2, BLK, BLK, 128), jnp.bfloat16),
            VMEM((16, cells), f32),
            pltpu.SemaphoreType.DMA,
        ],
        compiler_params=params,
        name="finish",
    )(*map(close, (local, *x_got, *y_got, *z_got, z_fix, loaded, harm, ids)))
    modes = lax.all_to_all(modes, AXES, 0, 0, tiled=True).sum(0)
    return psi, modes[: 2 * SPHERES, :MODES].reshape(SPHERES, 2, MODES)


def solution(mesh):
    in_specs = (
        P(None, "gx", "gy", "gz"),
        P(None, "gx", "gy", "gz"),
        P("gx", "gy", "gz", None, None),
        P("gx", "gy", "gz", None),
        P(),
        P(),
    )
    out_specs = (P(None, "gx", "gy", "gz"), P())
    return jax.shard_map(shards, mesh=mesh, in_specs=in_specs, out_specs=out_specs, check_vma=False)
```

```python
import functools
import math

import jax
import jax.numpy as jnp
import numpy as np
from jax import lax
from jax.experimental import pallas as pl
from jax.experimental.pallas import tpu as pltpu
from jax.sharding import PartitionSpec as P

BLK = 16
PTS = 2048
SPHERES = 3
LMAX = 8
AXES = ("gx", "gy", "gz")
MODES = (LMAX + 1) ** 2 - 4
ROWS = 24
NEAR = 1.0 / 3.0
FAR = 1.0 / 24.0
XX, XY, XZ, YY, YZ, ZZ = range(6)
VMEM = pltpu.VMEM
LIMIT = 24 * 1024 * 1024


def recurrence():
    table = np.zeros((ROWS, 128), np.float32)
    norm = lambda degree: math.sqrt((2 * degree + 1) / (4.0 * math.pi))
    for order in range(-LMAX, LMAX + 1):
        low = max(2, abs(order))
        row = order + LMAX
        gap = lambda degree: math.sqrt((degree**2 - order**2) * (degree**2 - 4))
        for degree in range(low, LMAX):
            base = 3 * (degree - 2)
            lift = degree * gap(degree + 1)
            scale = norm(degree + 1) / norm(degree) * (2 * degree + 1) / lift
            table[row, base] = scale * degree * (degree + 1)
            table[row, base + 1] = -scale * 2 * order
            if degree > low:
                table[row, base + 2] = norm(degree + 1) / norm(degree - 1) * (degree + 1) * gap(degree) / lift
        step = min(max(order, -2), 2) + 2 if low == 2 else (low + 2 if order > 0 else 0)
        lower = step - 2 - order
        lead = (-1.0) ** order * math.sqrt(
            math.factorial(low + order)
            * math.factorial(low - order)
            * (2 * low + 1)
            / (4.0 * math.pi * math.factorial(low - 2) * math.factorial(low + 2))
        )
        table[row, 127] = lead * math.comb(low + 2, step) * math.comb(low - 2, lower) * (-1.0) ** (low - step + 2)
    return table


def frame(x, y, z):
    rho2 = x * x + y * y
    inv_rho = lax.rsqrt(rho2)
    inv_r = lax.rsqrt(rho2 + z * z)
    cos_p = x * inv_rho
    sin_p = y * inv_rho
    cos_t = z * inv_r
    sin_t = rho2 * inv_rho * inv_r
    cc = cos_p * cos_p
    ss = sin_p * sin_p
    tt = cos_t * cos_t
    cs = cos_p * sin_p
    st = sin_t * cos_t
    twice_p = (tt * cc - ss, cs * (tt + 1.0), -(st * cos_p), tt * ss - cc, -(st * sin_p), sin_t * sin_t)
    q_diag = cos_t * cs
    twice_q = (cos_t * (cc - ss), sin_t * sin_p, -(sin_t * cos_p))
    return twice_p, q_diag, twice_q


def total(terms):
    terms = [term for term in terms if term is not None]
    return functools.reduce(lambda one, two: one + two, terms)


def times(one, two):
    return None if one is None or two is None else one * two


def minus(one, two):
    if two is None:
        return one
    return -two if one is None else one - two


def contract(geometry, electric, magnetic):
    twice_p, q_diag, twice_q = geometry
    e, b = electric, magnetic
    half = total([times(twice_p[i], e[i]) for i in (XX, YY, ZZ)]) * 0.5
    real_e = half + total([times(twice_p[i], e[i]) for i in (XY, XZ, YZ)])
    off = (XY, XZ, YZ)
    imag_e = q_diag * (e[YY] - e[XX]) + total([twice_q[n] * e[i] for n, i in enumerate(off)])
    real_b = total([times(2.0 * q_diag, minus(b[YY], b[XX]))] + [times(twice_q[n], b[i]) for n, i in enumerate(off)])
    imag_b = total([times(twice_p[i], b[i]) for i in range(6)])
    return real_e - real_b, -(imag_e + imag_b)


def curl_part(axis, d):
    yz, xz, xy, diff = d
    if axis == 0:
        return [None, -xz, xy, -yz, diff, yz]
    if axis == 1:
        return [xz, yz, diff, None, -xy, -xz]
    return [-xy, diff, -yz, xy, xz, None]


DIFFS = ((YY, ZZ), (ZZ, XX), (XX, YY))


def iota(shape, dim):
    return lax.broadcasted_iota(jnp.int32, shape, dim)


def origin(axis, cells):
    place = lax.axis_index(axis)
    count = lax.axis_size(axis)
    return (place * cells).astype(jnp.float32) + (0.5 - count * cells / 2.0), place


def face_part(axis, near, far, sign, geometry):
    h_near, k_near = near if near is not None else (None, None)
    h_far, k_far = far
    if near is None:
        e = [h * FAR for h in h_far]
        d = [k * (-FAR * sign) for k in k_far]
    else:
        e = [f * FAR - n * (2.0 / 3.0) for n, f in zip(h_near, h_far)]
        d = [(n * NEAR - f * FAR) * sign for n, f in zip(k_near, k_far)]
    return contract(geometry, e, curl_part(axis, d))


def pick_k(axis, load):
    one, two = DIFFS[axis]
    return [load(6 + YZ), load(6 + XZ), load(6 + XY), load(6 + one) - load(6 + two)]


def upward(place, slots, slot):
    return place == 0 if slots == 1 else jnp.asarray(slot == 0)


def faces_kernel(slots, metric, curvature, *refs):
    nx = slots[0]
    ny = slots[1]
    x_out = refs[:nx]
    y_out = refs[nx : nx + ny]
    z_out, z_fix, fields, sems = refs[nx + ny :]
    copies = []
    for comp in range(6):
        for base, source in ((0, metric), (6, curvature)):
            copies.append(
                pltpu.make_async_copy(
                    source.at[comp],
                    fields.at[base + comp, pl.ds(2, BLK), pl.ds(8, BLK), :],
                    sems.at[base + comp],
                )
            )
    for copy in copies:
        copy.start()
    blank = jnp.zeros((12, BLK, 8, 128), jnp.float32)
    fields[:, pl.ds(2, BLK), pl.ds(0, 8), :] = blank
    fields[:, pl.ds(2, BLK), pl.ds(24, 8), :] = blank
    plane = jnp.zeros((12, 2, BLK, 128), jnp.float32)
    fields[:, pl.ds(0, 2), pl.ds(8, BLK), :] = plane
    fields[:, pl.ds(BLK + 2, 2), pl.ds(8, BLK), :] = plane
    for copy in copies:
        copy.wait()
    x0, ix = origin("gx", BLK)
    y0, iy = origin("gy", BLK)
    z0, iz = origin("gz", 128)
    slab = (BLK, 128)
    rows = iota(slab, 0).astype(jnp.float32)
    lanes = iota(slab, 1).astype(jnp.float32)
    z = lanes + z0
    for slot in range(nx):
        high = upward(ix, nx, slot)
        near_at = jnp.where(high, BLK + 1, 2)
        far_at = jnp.where(high, BLK, 3)
        sign = jnp.where(high, -1.0, 1.0)
        near = [fields[c, near_at, pl.ds(8, BLK), :] for c in range(6)]
        far = [fields[c, far_at, pl.ds(8, BLK), :] for c in range(6)]
        k_near = pick_k(0, lambda c: fields[c, near_at, pl.ds(8, BLK), :])
        k_far = pick_k(0, lambda c: fields[c, far_at, pl.ds(8, BLK), :])
        y = rows + y0
        for layer in range(2):
            x = jnp.where(high, x0 + (BLK + layer), x0 - (1 + layer))
            geometry = frame(x, y, z)
            if layer == 0:
                real, imag = face_part(0, (near, k_near), (far, k_far), sign, geometry)
            else:
                real, imag = face_part(0, None, (near, k_near), sign, geometry)
            x_out[slot][0, layer] = real
            x_out[slot][1, layer] = imag
    for slot in range(ny):
        high = upward(iy, ny, slot)
        near_at = jnp.where(high, 8 + BLK - 1, 8)
        far_at = jnp.where(high, 8 + BLK - 2, 9)
        sign = jnp.where(high, -1.0, 1.0)

        def line(c, at):
            return fields.reshape(12 * 20 * 32, 128)[pl.ds(c * 640 + 64 + at, BLK, stride=32), :]

        near = [line(c, near_at) for c in range(6)]
        far = [line(c, far_at) for c in range(6)]
        k_near = pick_k(1, lambda c: line(c, near_at))
        k_far = pick_k(1, lambda c: line(c, far_at))
        x = rows + x0
        for layer in range(2):
            y = jnp.where(high, y0 + (BLK + layer), y0 - (1 + layer))
            geometry = frame(x, y, z)
            if layer == 0:
                real, imag = face_part(1, (near, k_near), (far, k_far), sign, geometry)
            else:
                real, imag = face_part(1, None, (near, k_near), sign, geometry)
            y_out[slot][0, layer] = real
            y_out[slot][1, layer] = imag
    lane = iota((8, 128), 1)
    group = lane // 4

    def packed(load):
        out = jnp.zeros((8, 128), jnp.float32)
        for j in range(32):
            value = load(j // 2, j % 2)
            out = jnp.where(group == j, pltpu.roll(value, (2 + 4 * j) % 128, 1), out)
        return out

    def piece(c):
        return lambda x, half: fields[c, 2 + x, pl.ds(8 + 8 * half, 8), :]

    h_all = [packed(piece(c)) for c in range(6)]
    one, two = DIFFS[2]
    k_all = [packed(piece(6 + c)) for c in (YZ, XZ, XY)]
    k_all.append(packed(lambda x, half: piece(6 + one)(x, half) - piece(6 + two)(x, half)))
    q = lane % 4
    upper = q >= 2
    inner = (q == 1) | (q == 2)

    def shifted(value, by):
        return jnp.where(upper, pltpu.roll(value, by, 1), pltpu.roll(value, 128 - by, 1))

    e = [shifted(h, 2) * FAR - jnp.where(inner, shifted(h, 1), 0.0) * (2.0 / 3.0) for h in h_all]
    sign = jnp.where(upper, -1.0, 1.0)
    d = [(jnp.where(inner, shifted(k, 1), 0.0) * NEAR - shifted(k, 2) * FAR) * sign for k in k_all]
    magnetic = curl_part(2, d)
    x = (lane // 8).astype(jnp.float32) + x0
    y = (iota((8, 128), 0) + 8 * (group % 2)).astype(jnp.float32) + y0
    z_here = jnp.where(upper, q - 2, q + 126).astype(jnp.float32) + z0
    z_there = z_here + jnp.where(upper, 128.0, -128.0)
    for out, z_at in ((z_out, z_there), (z_fix, z_here)):
        real, imag = contract(frame(x, y, z_at), e, magnetic)
        out[0] = real
        out[1] = imag


def sin_cos(x):
    x2 = x * x
    sine = 0.0
    cosine = 0.0
    for n in range(6, -1, -1):
        sine = sine * x2 + (-1.0) ** n / math.factorial(2 * n + 1)
    for n in range(7, -1, -1):
        cosine = cosine * x2 + (-1.0) ** n / math.factorial(2 * n)
    return sine * x, cosine


def split3(value):
    one = value.astype(jnp.bfloat16)
    rest = value - one.astype(jnp.float32)
    two = rest.astype(jnp.bfloat16)
    three = (rest - two.astype(jnp.float32)).astype(jnp.bfloat16)
    return one, two, three


def interior_kernel(fields, ids_far, theta_far, phi_far, coefs_far, weights, local, harm, ids, loaded, *scratch):
    lists, theta, phi, coefs, sems = scratch
    small = [
        pltpu.make_async_copy(source, target, sems.at[n])
        for n, (source, target) in enumerate(
            ((ids_far, lists), (theta_far, theta), (phi_far, phi), (coefs_far, coefs))
        )
    ]
    copy = pltpu.make_async_copy(weights, loaded, sems.at[4])
    for each in small:
        each.start()
    copy.start()
    x0, _ = origin("gx", BLK)
    y0, _ = origin("gy", BLK)
    z0, _ = origin("gz", 128)
    slab = (BLK, 128)
    y = iota(slab, 0).astype(jnp.float32) + y0
    z = iota(slab, 1).astype(jnp.float32) + z0

    def plane(i, carry):
        def at(c, dx=0, dy=0):
            return fields[c, i + (2 + dx), pl.ds(8 + dy, BLK), :]

        def roll(value, by):
            return pltpu.roll(value, by % 128, 1)

        geometry = frame(x0 + i.astype(jnp.float32), y, z)
        k = [at(6 + c) for c in range(6)]
        trace = k[XX] + k[YY] + k[ZZ]
        prod = {}

        def mul(a, b):
            key = (min(a, b), max(a, b))
            if key not in prod:
                prod[key] = k[key[0]] * k[key[1]]
            return prod[key]

        pairs = ((XX, XY, XZ), (XY, YY, YZ), (XZ, YZ, ZZ))
        e = []
        for row in range(3):
            for col in range(row, 3):
                c = pairs[row][col]
                h = at(c)
                one = (at(c, -1) + at(c, 1)) + (at(c, 0, -1) + at(c, 0, 1)) + (roll(h, 1) + roll(h, -1))
                two = (at(c, -2) + at(c, 2)) + (at(c, 0, -2) + at(c, 0, 2)) + (roll(h, 2) + roll(h, -2))
                square = total([mul(pairs[row][n], pairs[n][col]) for n in range(3)])
                e.append(two * FAR - one * (2.0 / 3.0) + h * 3.75 + (trace * k[c] - square))

        def slope(m2, m1, p1, p2):
            return (p1 - m1) * NEAR - (p2 - m2) * FAR

        steps = (-2, -1, 1, 2)
        along_x = [pick_k(0, lambda c, s=s: at(c, s)) for s in steps]
        dx = [slope(*[along_x[n][f] for n in range(4)]) for f in range(4)]
        along_y = [pick_k(1, lambda c, s=s: at(c, 0, s)) for s in steps]
        dy = [slope(*[along_y[n][f] for n in range(4)]) for f in range(4)]
        here = [k[YZ], k[XZ], k[XY], k[XX] - k[YY]]
        dz = [slope(*[roll(f, -s) for s in steps]) for f in here]
        parts = [curl_part(axis, d) for axis, d in enumerate((dx, dy, dz))]
        magnetic = [total([part[c] for part in parts]) for c in range(6)]
        real, imag = contract(geometry, e, magnetic)
        local[0, i] = real
        local[1, i] = imag
        return carry

    lax.fori_loop(0, BLK, plane, 0)
    for each in small:
        each.wait()
    count = ids.shape[1]
    id_row = jnp.concatenate([lists[n : n + 1] for n in range(lists.shape[0])], axis=1)
    ids[...] = id_row
    wide = (theta.shape[0], count)
    pick = jnp.where(iota(wide, 0) == id_row // 128, 1.0, 0.0).astype(jnp.bfloat16)
    tables = jnp.concatenate([theta[...], phi[...]], axis=1)
    left = jnp.concatenate(split3(tables), axis=0)
    right = jnp.concatenate([pick] * 3, axis=0)
    found = lax.dot_general(left, right, (((0,), (0,)), ((), ())), preferred_element_type=jnp.float32)
    mine = iota((128, count), 0) == id_row % 128
    half_t = jnp.sum(jnp.where(mine, found[:128], 0.0), axis=0, keepdims=True) * 0.5
    half_p = jnp.sum(jnp.where(mine, found[128:], 0.0), axis=0, keepdims=True) * 0.5
    sines, cosines = sin_cos(jnp.concatenate([half_t, half_p, jnp.zeros((6, count), jnp.float32)], axis=0))
    sin_h, cos_h = sines[0:1], cosines[0:1]
    cos_t = cos_h * cos_h - sin_h * sin_h
    sin_p = 2.0 * sines[1:2] * cosines[1:2]
    cos_p = 1.0 - 2.0 * sines[1:2] * sines[1:2]
    shape = (ROWS, count)
    order = iota(shape, 0) - LMAX
    size = jnp.abs(order)
    lowest = jnp.maximum(size, 2)
    tilt = jnp.clip(order, -2, 2)
    unit_r = jnp.ones(shape, jnp.float32)
    unit_i = jnp.zeros(shape, jnp.float32)
    start = jnp.where(size <= LMAX, coefs[:, 127:128], 0.0)
    step_r, step_i, step_c, step_s = cos_p, sin_p, cos_h, sin_h
    for bit in range(4):
        has = (size >> bit) & 1 == 1
        new_r = unit_r * step_r - unit_i * step_i
        new_i = unit_r * step_i + unit_i * step_r
        unit_r = jnp.where(has, new_r, unit_r)
        unit_i = jnp.where(has, new_i, unit_i)
        start = jnp.where(((lowest + tilt) >> bit) & 1 == 1, start * step_c, start)
        start = jnp.where(((lowest - tilt) >> bit) & 1 == 1, start * step_s, start)
        step_r, step_i = step_r * step_r - step_i * step_i, 2.0 * step_r * step_i
        step_c = step_c * step_c
        step_s = step_s * step_s
    unit_i = jnp.where(order < 0, -unit_i, unit_i)
    before = jnp.zeros(shape, jnp.float32)
    now = jnp.where(lowest == 2, start, 0.0)
    for degree in range(2, LMAX + 1):
        if degree > 2:
            base = 3 * (degree - 3)
            slope = coefs[:, base : base + 1] * cos_t + coefs[:, base + 1 : base + 2]
            after = slope * now - coefs[:, base + 2 : base + 3] * before
            before, now = now, jnp.where(lowest == degree, start, after)
        at = degree * degree - 4
        width = 2 * degree + 1
        low = LMAX - degree
        harm[pl.ds(at, width), pl.ds(0, count)] = (now * unit_r)[low : low + width]
        harm[pl.ds(at, width), pl.ds(count, count)] = (now * unit_i)[low : low + width]
    harm[pl.ds(MODES, 80 - MODES), :] = jnp.zeros((80 - MODES, 2 * count), jnp.float32)
    copy.wait()


def below(place, slots, slot, axis):
    if slots == 1:
        return place == 1, jnp.asarray(True)
    return jnp.asarray(slot == 0), (place > 0 if slot == 0 else place < lax.axis_size(axis) - 1)


def finish_kernel(slots, local, *refs):
    nx, ny, nz = slots
    x_in = refs[:nx]
    y_in = refs[nx : nx + ny]
    z_in = refs[nx + ny : nx + ny + nz]
    z_fix, weights, harm, ids, psi, modes, work, stored, flat, sem = refs[nx + ny + nz :]
    ix = lax.axis_index("gx")
    iy = lax.axis_index("gy")
    iz = lax.axis_index("gz")
    lane = iota((8, 128), 1)
    q = lane % 4
    edge = (lane >= 126) | (lane < 2)
    upper = q < 2
    held = jnp.where(upper, (iz < lax.axis_size("gz") - 1).astype(jnp.int32), (iz > 0).astype(jnp.int32)) == 1
    for part in range(2):
        z_part = jnp.where(upper, z_in[-1][part], z_in[0][part])
        z_part = jnp.where(held, z_part, 0.0) - z_fix[part]
        for j in range(32):
            moved = pltpu.roll(z_part, (126 - 4 * j) % 128, 1)
            value = local[part, j // 2, pl.ds(8 * (j % 2), 8), :]
            work[part, pl.ds(8 * j, 8), :] = value + jnp.where(edge, moved, 0.0)
    for part in range(2):
        for slot in range(nx):
            low, real = below(ix, nx, slot, "gx")
            for layer in range(2):
                at = jnp.where(low, layer, BLK - 1 - layer) * BLK
                span = pl.ds(pl.multiple_of(at, BLK), BLK)
                work[part, span, :] = work[part, span, :] + jnp.where(real, x_in[slot][part, layer], 0.0)
        for slot in range(ny):
            low, real = below(iy, ny, slot, "gy")
            for layer in range(2):
                at = jnp.where(low, layer, BLK - 1 - layer)
                span = pl.ds(part * 256 + at, BLK, stride=BLK)
                both = work.reshape(512, 128)
                both[span, :] = both[span, :] + jnp.where(real, y_in[slot][part, layer], 0.0)
    row = iota((8, 128), 0)
    source = (lane // BLK + row + 1) % 8
    for part in range(2):
        for x in range(BLK):
            rounded = work[part, pl.ds(BLK * x, BLK), :].astype(jnp.bfloat16)
            stored[part, x] = rounded
            values = rounded.astype(jnp.float32)
            for half in range(2):
                value = values[8 * half : 8 * half + 8]
                value = pltpu.roll(value, 0, 1, stride=BLK, stride_axis=0)
                value = jnp.take_along_axis(value, source, axis=0)
                value = pltpu.roll(value, BLK, 1, stride=BLK, stride_axis=0)
                flat[pl.ds(8 * part, 8), pl.ds((2 * x + half) * 128, 128)] = value
    copy = pltpu.make_async_copy(stored, psi, sem)
    copy.start()
    count = ids.shape[1]
    blocks = flat[...].astype(jnp.bfloat16)
    product = lax.dot_general(
        blocks, weights[...], (((1,), (1,)), ((), ())), preferred_element_type=jnp.float32
    )
    own = iota((8, count), 0) == 7 - iota((8, count), 1) // (count // 8)
    real = jnp.sum(jnp.where(own, product[:8], 0.0), axis=0, keepdims=True)
    imag = jnp.sum(jnp.where(own, product[8:], 0.0), axis=0, keepdims=True)
    row = iota((8, count), 0)
    live = ids[...] // PTS == row // 2
    first = row % 2 == 0
    left = jnp.where(live, jnp.where(first, real, imag), 0.0)
    right = jnp.where(live, jnp.where(first, imag, -real), 0.0)
    sums = lax.dot_general(
        jnp.concatenate([left, right], axis=1),
        harm[...],
        (((1,), (1,)), ((), ())),
        precision=lax.Precision.HIGHEST,
        preferred_element_type=jnp.float32,
    )
    sums = sums * (4.0 * math.pi / PTS)
    sums = jnp.concatenate([sums, jnp.zeros((8, 128 - 80), jnp.float32)], axis=1)
    modes[...] = jnp.broadcast_to(sums[None], modes.shape)
    copy.wait()


def shift(axis, slot):
    count = lax.axis_size(axis)
    step = 1 - 2 * slot
    return [(place, (place + step) % count) for place in range(count)]


def shards(metric_pert, curvature, interp_weights, point_ids, theta, phi):
    f32 = jnp.float32
    hbm = pl.BlockSpec(memory_space=pltpu.HBM)
    far = lambda value: pltpu.with_memory_space_constraint(value, pltpu.HBM)
    close = lambda value: pltpu.with_memory_space_constraint(value, VMEM)
    vmem = pl.BlockSpec(memory_space=VMEM)
    slots = tuple(min(2, lax.axis_size(axis) - 1) for axis in AXES)
    nx, ny, nz = slots
    count = point_ids.size
    lists = point_ids.shape[2:]
    cells = BLK * BLK * BLK
    face = VMEM((2, 2, BLK, 128), f32)
    edge = VMEM((2, 8, 128), f32)
    params = pltpu.CompilerParams(vmem_limit_bytes=LIMIT)
    first = pl.pallas_call(
        functools.partial(faces_kernel, slots),
        out_shape=[face] * (nx + ny) + [edge, edge, VMEM((12, 20, 32, 128), f32)],
        in_specs=[hbm] * 2,
        out_specs=[vmem] * (nx + ny + 3),
        scratch_shapes=[pltpu.SemaphoreType.DMA((12,))],
        compiler_params=params,
        name="faces",
    )(far(metric_pert), far(curvature))
    x_send, y_send = first[:nx], first[nx : nx + ny]
    z_send, z_fix, fields = first[nx + ny :]
    x_got = [lax.ppermute(x_send[slot], "gx", shift("gx", slot)) for slot in range(nx)]
    y_got = [lax.ppermute(y_send[slot], "gy", shift("gy", slot)) for slot in range(ny)]
    z_got = [lax.ppermute(z_send, "gz", shift("gz", slot)) for slot in range(nz)]
    weights = interp_weights.reshape(count, cells)
    local, harm, ids, loaded = pl.pallas_call(
        interior_kernel,
        out_shape=[VMEM((2, BLK, BLK, 128), f32), VMEM((80, 2 * count), f32), VMEM((1, count), jnp.int32), VMEM((count, cells), jnp.bfloat16)],
        in_specs=[vmem] + [hbm] * 5,
        out_specs=[vmem] * 4,
        scratch_shapes=[
            VMEM(lists, jnp.int32),
            VMEM((theta.size // 128, 128), f32),
            VMEM((theta.size // 128, 128), f32),
            VMEM((ROWS, 128), f32),
            pltpu.SemaphoreType.DMA((5,)),
        ],
        compiler_params=params,
        cost_estimate=pl.CostEstimate(flops=20_000_000, bytes_accessed=8_000_000, transcendentals=0),
        name="interior",
    )(
        close(fields),
        far(point_ids.reshape(lists)),
        far(theta.reshape(-1, 128)),
        far(phi.reshape(-1, 128)),
        far(jnp.asarray(recurrence())),
        far(weights),
    )
    total_devices = math.prod(lax.axis_size(axis) for axis in AXES)
    psi, modes = pl.pallas_call(
        functools.partial(finish_kernel, slots),
        out_shape=[pltpu.HBM((2, BLK, BLK, 128), jnp.bfloat16), VMEM((total_devices, 8, 128), f32)],
        in_specs=[vmem] * (1 + nx + ny + nz + 4),
        out_specs=[hbm, vmem],
        scratch_shapes=[
            VMEM((2, 256, 128), f32),
            VMEM((2, BLK, BLK, 128), jnp.bfloat16),
            VMEM((16, cells), f32),
            pltpu.SemaphoreType.DMA,
        ],
        compiler_params=params,
        name="finish",
    )(*map(close, (local, *x_got, *y_got, *z_got, z_fix, loaded, harm, ids)))
    modes = lax.all_to_all(modes, AXES, 0, 0, tiled=True).sum(0)
    return psi, modes[: 2 * SPHERES, :MODES].reshape(SPHERES, 2, MODES)


def solution(mesh):
    in_specs = (
        P(None, "gx", "gy", "gz"),
        P(None, "gx", "gy", "gz"),
        P("gx", "gy", "gz", None, None),
        P("gx", "gy", "gz", None),
        P(),
        P(),
    )
    out_specs = (P(None, "gx", "gy", "gz"), P())
    return jax.shard_map(shards, mesh=mesh, in_specs=in_specs, out_specs=out_specs, check_vma=False)
```

```python
import functools
import math

import jax
import jax.numpy as jnp
import numpy as np
from jax import lax
from jax.experimental import pallas as pl
from jax.experimental.pallas import tpu as pltpu
from jax.sharding import PartitionSpec as P

BLK = 16
PTS = 2048
SPHERES = 3
LMAX = 8
AXES = ("gx", "gy", "gz")
MODES = (LMAX + 1) ** 2 - 4
ROWS = 24
NEAR = 1.0 / 3.0
FAR = 1.0 / 24.0
XX, XY, XZ, YY, YZ, ZZ = range(6)
VMEM = pltpu.VMEM
LIMIT = 24 * 1024 * 1024


def recurrence():
    table = np.zeros((ROWS, 128), np.float32)
    norm = lambda degree: math.sqrt((2 * degree + 1) / (4.0 * math.pi))
    for order in range(-LMAX, LMAX + 1):
        low = max(2, abs(order))
        row = order + LMAX
        gap = lambda degree: math.sqrt((degree**2 - order**2) * (degree**2 - 4))
        for degree in range(low, LMAX):
            base = 3 * (degree - 2)
            lift = degree * gap(degree + 1)
            scale = norm(degree + 1) / norm(degree) * (2 * degree + 1) / lift
            table[row, base] = scale * degree * (degree + 1)
            table[row, base + 1] = -scale * 2 * order
            if degree > low:
                table[row, base + 2] = norm(degree + 1) / norm(degree - 1) * (degree + 1) * gap(degree) / lift
        step = min(max(order, -2), 2) + 2 if low == 2 else (low + 2 if order > 0 else 0)
        lower = step - 2 - order
        lead = (-1.0) ** order * math.sqrt(
            math.factorial(low + order)
            * math.factorial(low - order)
            * (2 * low + 1)
            / (4.0 * math.pi * math.factorial(low - 2) * math.factorial(low + 2))
        )
        table[row, 127] = lead * math.comb(low + 2, step) * math.comb(low - 2, lower) * (-1.0) ** (low - step + 2)
    return table


def frame(x, y, z):
    rho2 = x * x + y * y
    inv_rho = lax.rsqrt(rho2)
    inv_r = lax.rsqrt(rho2 + z * z)
    cos_p = x * inv_rho
    sin_p = y * inv_rho
    cos_t = z * inv_r
    sin_t = rho2 * inv_rho * inv_r
    cc = cos_p * cos_p
    ss = sin_p * sin_p
    tt = cos_t * cos_t
    cs = cos_p * sin_p
    st = sin_t * cos_t
    twice_p = (tt * cc - ss, cs * (tt + 1.0), -(st * cos_p), tt * ss - cc, -(st * sin_p), sin_t * sin_t)
    q_diag = cos_t * cs
    twice_q = (cos_t * (cc - ss), sin_t * sin_p, -(sin_t * cos_p))
    return twice_p, q_diag, twice_q


def total(terms):
    terms = [term for term in terms if term is not None]
    return functools.reduce(lambda one, two: one + two, terms)


def times(one, two):
    return None if one is None or two is None else one * two


def minus(one, two):
    if two is None:
        return one
    return -two if one is None else one - two


def contract(geometry, electric, magnetic):
    twice_p, q_diag, twice_q = geometry
    e, b = electric, magnetic
    off = (XY, XZ, YZ)
    real_e = (twice_p[XX] * e[0] + twice_p[YY] * e[1]) * 0.5
    real_e = real_e + total([twice_p[i] * e[2 + n] for n, i in enumerate(off)])
    imag_e = q_diag * (e[1] - e[0]) + total([twice_q[n] * e[2 + n] for n in range(3)])
    real_b = total([times(2.0 * q_diag, minus(b[YY], b[XX]))] + [times(twice_q[n], b[i]) for n, i in enumerate(off)])
    imag_b = total([times(twice_p[i], b[i]) for i in range(6)])
    return real_e - real_b, -(imag_e + imag_b)


def curl_part(axis, d):
    yz, xz, xy, diff = d
    if axis == 0:
        return [None, -xz, xy, -yz, diff, yz]
    if axis == 1:
        return [xz, yz, diff, None, -xy, -xz]
    return [-xy, diff, -yz, xy, xz, None]


H_PARTS = (XX, YY, XY, XZ, YZ)
DIFFS = ((YY, ZZ), (ZZ, XX), (XX, YY))


def iota(shape, dim):
    return lax.broadcasted_iota(jnp.int32, shape, dim)


def origin(axis, cells):
    place = lax.axis_index(axis)
    count = lax.axis_size(axis)
    return (place * cells).astype(jnp.float32) + (0.5 - count * cells / 2.0), place


def face_part(axis, near, far, sign, geometry):
    h_near, k_near = near if near is not None else (None, None)
    h_far, k_far = far
    if near is None:
        e = [h * FAR for h in h_far]
        d = [k * (-FAR * sign) for k in k_far]
    else:
        e = [f * FAR - n * (2.0 / 3.0) for n, f in zip(h_near, h_far)]
        d = [(n * NEAR - f * FAR) * sign for n, f in zip(k_near, k_far)]
    return contract(geometry, e, curl_part(axis, d))


def pick_k(axis, load):
    one, two = DIFFS[axis]
    return [load(6 + YZ), load(6 + XZ), load(6 + XY), load(6 + one) - load(6 + two)]


def sin_cos(x):
    x2 = x * x
    sine = 0.0
    cosine = 0.0
    for n in range(6, -1, -1):
        sine = sine * x2 + (-1.0) ** n / math.factorial(2 * n + 1)
    for n in range(7, -1, -1):
        cosine = cosine * x2 + (-1.0) ** n / math.factorial(2 * n)
    return sine * x, cosine


def split3(value):
    one = value.astype(jnp.bfloat16)
    rest = value - one.astype(jnp.float32)
    two = rest.astype(jnp.bfloat16)
    three = (rest - two.astype(jnp.float32)).astype(jnp.bfloat16)
    return one, two, three


def harmonics(lists, theta, phi, coefs, plain, harm, ids):
    count = ids.shape[1]
    id_row = jnp.concatenate([lists[n : n + 1] for n in range(lists.shape[0])], axis=1)
    ids[...] = id_row
    wide = (theta.shape[0], count)
    pick = jnp.where(iota(wide, 0) == id_row // 128, 1.0, 0.0).astype(jnp.bfloat16)
    tables = jnp.concatenate([theta[...], phi[...]], axis=1)
    left = jnp.concatenate(split3(tables), axis=0)
    right = jnp.concatenate([pick] * 3, axis=0)
    found = lax.dot_general(left, right, (((0,), (0,)), ((), ())), preferred_element_type=jnp.float32)
    mine = iota((128, count), 0) == id_row % 128
    half_t = jnp.sum(jnp.where(mine, found[:128], 0.0), axis=0, keepdims=True) * 0.5
    half_p = jnp.sum(jnp.where(mine, found[128:], 0.0), axis=0, keepdims=True) * 0.5
    sines, cosines = sin_cos(jnp.concatenate([half_t, half_p, jnp.zeros((6, count), jnp.float32)], axis=0))
    sin_h, cos_h = sines[0:1], cosines[0:1]
    cos_t = cos_h * cos_h - sin_h * sin_h
    sin_p = 2.0 * sines[1:2] * cosines[1:2]
    cos_p = 1.0 - 2.0 * sines[1:2] * sines[1:2]
    shape = (ROWS, count)
    order = iota(shape, 0) - LMAX
    size = jnp.abs(order)
    lowest = jnp.maximum(size, 2)
    tilt = jnp.clip(order, -2, 2)
    unit_r = jnp.ones(shape, jnp.float32)
    unit_i = jnp.zeros(shape, jnp.float32)
    start = jnp.where(size <= LMAX, coefs[:, 127:128], 0.0)
    step_r, step_i, step_c, step_s = cos_p, sin_p, cos_h, sin_h
    for bit in range(4):
        has = (size >> bit) & 1 == 1
        new_r = unit_r * step_r - unit_i * step_i
        new_i = unit_r * step_i + unit_i * step_r
        unit_r = jnp.where(has, new_r, unit_r)
        unit_i = jnp.where(has, new_i, unit_i)
        start = jnp.where(((lowest + tilt) >> bit) & 1 == 1, start * step_c, start)
        start = jnp.where(((lowest - tilt) >> bit) & 1 == 1, start * step_s, start)
        step_r, step_i = step_r * step_r - step_i * step_i, 2.0 * step_r * step_i
        step_c = step_c * step_c
        step_s = step_s * step_s
    unit_i = jnp.where(order < 0, -unit_i, unit_i)
    before = jnp.zeros(shape, jnp.float32)
    now = jnp.where(lowest == 2, start, 0.0)
    for degree in range(2, LMAX + 1):
        if degree > 2:
            base = 3 * (degree - 3)
            slope = coefs[:, base : base + 1] * cos_t + coefs[:, base + 1 : base + 2]
            after = slope * now - coefs[:, base + 2 : base + 3] * before
            before, now = now, jnp.where(lowest == degree, start, after)
        at = degree * degree - 4
        width = 2 * degree + 1
        low = LMAX - degree
        plain[pl.ds(at, width), pl.ds(0, count)] = (now * unit_r)[low : low + width]
        plain[pl.ds(at, width), pl.ds(count, count)] = (now * unit_i)[low : low + width]
    plain[pl.ds(MODES, 80 - MODES), :] = jnp.zeros((80 - MODES, 2 * count), jnp.float32)
    whole = plain[...]
    main = whole.astype(jnp.bfloat16)
    harm[0] = main
    harm[1] = (whole - main.astype(jnp.float32)).astype(jnp.bfloat16)


def faces_kernel(slots, metric, curvature, ids_far, theta_far, phi_far, coefs_far, *refs):
    nx, ny, _ = slots
    x_out = refs[:nx]
    y_out = refs[nx : nx + ny]
    z_out, z_fix, fields, harm, ids, lists, theta, phi, coefs, plain, sems = refs[nx + ny :]
    small = [
        pltpu.make_async_copy(source, target, sems.at[n])
        for n, (source, target) in enumerate(
            ((ids_far, lists), (theta_far, theta), (phi_far, phi), (coefs_far, coefs))
        )
    ]
    copies = []
    for base, source in ((0, metric), (6, curvature)):
        copies.append(
            pltpu.make_async_copy(
                source,
                fields.at[pl.ds(base, 6), pl.ds(2, BLK), pl.ds(8, BLK), :],
                sems.at[4 + base // 6],
            )
        )
    for copy in small + copies:
        copy.start()
    blank = jnp.zeros((12, BLK, 8, 128), jnp.float32)
    fields[:, pl.ds(2, BLK), pl.ds(0, 8), :] = blank
    fields[:, pl.ds(2, BLK), pl.ds(24, 8), :] = blank
    plane = jnp.zeros((12, 2, BLK, 128), jnp.float32)
    fields[:, pl.ds(0, 2), pl.ds(8, BLK), :] = plane
    fields[:, pl.ds(BLK + 2, 2), pl.ds(8, BLK), :] = plane
    for copy in small:
        copy.wait()
    harmonics(lists, theta, phi, coefs, plain, harm, ids)
    for copy in copies:
        copy.wait()
    inside = (pl.ds(2, BLK), pl.ds(8, BLK), slice(None))
    h_zz = fields[(ZZ, *inside)]
    fields[(XX, *inside)] = fields[(XX, *inside)] - h_zz
    fields[(YY, *inside)] = fields[(YY, *inside)] - h_zz
    x0, ix = origin("gx", BLK)
    y0, iy = origin("gy", BLK)
    z0, iz = origin("gz", 128)
    slab = (BLK, 128)
    rows = iota(slab, 0).astype(jnp.float32)
    lanes = iota(slab, 1).astype(jnp.float32)
    z = lanes + z0

    def facing(axis, load, near_at, far_at, sign, geometry_at):
        near = [load(c, near_at) for c in H_PARTS]
        far = [load(c, far_at) for c in H_PARTS]
        k_near = pick_k(axis, lambda c: load(c, near_at))
        k_far = pick_k(axis, lambda c: load(c, far_at))
        return (
            face_part(axis, (near, k_near), (far, k_far), sign, geometry_at(0)),
            face_part(axis, None, (near, k_near), sign, geometry_at(1)),
        )

    def send(axis, place, outs, load, last, start, geometry):
        even = place % 2 == 0
        if len(outs) == 1:
            sides = [
                facing(
                    axis,
                    load,
                    jnp.where(even, last, 0),
                    jnp.where(even, last - 1, 1),
                    jnp.where(even, -1.0, 1.0),
                    lambda layer: geometry(jnp.where(even, start + (BLK + layer), start - (1 + layer))),
                )
            ]
        else:
            high = facing(axis, load, last, last - 1, -1.0, lambda layer: geometry(start + (BLK + layer)))
            low = facing(axis, load, 0, 1, 1.0, lambda layer: geometry(start - (1 + layer)))
            pick = lambda one, two: jax.tree.map(lambda a, b: jnp.where(even, a, b), one, two)
            sides = [pick(high, low), pick(low, high)]
        for out, side in zip(outs, sides):
            for layer in range(2):
                for part in range(2):
                    out[part, layer] = side[layer][part]

    flat = fields.reshape(12 * 20 * 32, 128)
    send(
        0,
        ix,
        x_out,
        lambda c, at: fields[c, 2 + at, pl.ds(8, BLK), :],
        BLK - 1,
        x0,
        lambda x: frame(x, rows + y0, z),
    )
    send(
        1,
        iy,
        y_out,
        lambda c, at: flat[pl.ds(c * 640 + 72 + at, BLK, stride=32), :],
        BLK - 1,
        y0,
        lambda y: frame(rows + x0, y, z),
    )
    lane = iota((8, 128), 1)
    group = lane // 4

    def packed(load):
        out = jnp.zeros((8, 128), jnp.float32)
        for j in range(32):
            value = load(j // 2, j % 2)
            out = jnp.where(group == j, pltpu.roll(value, (2 + 4 * j) % 128, 1), out)
        return out

    def piece(c):
        return lambda x, half: fields[c, 2 + x, pl.ds(8 + 8 * half, 8), :]

    h_all = [packed(piece(c)) for c in H_PARTS]
    one, two = DIFFS[2]
    k_all = [packed(piece(6 + c)) for c in (YZ, XZ, XY)]
    k_all.append(packed(lambda x, half: piece(6 + one)(x, half) - piece(6 + two)(x, half)))
    q = lane % 4
    upper = q >= 2
    inner = (q == 1) | (q == 2)

    def shifted(value, by):
        return jnp.where(upper, pltpu.roll(value, by, 1), pltpu.roll(value, 128 - by, 1))

    e = [shifted(h, 2) * FAR - jnp.where(inner, shifted(h, 1), 0.0) * (2.0 / 3.0) for h in h_all]
    sign = jnp.where(upper, -1.0, 1.0)
    d = [(jnp.where(inner, shifted(k, 1), 0.0) * NEAR - shifted(k, 2) * FAR) * sign for k in k_all]
    magnetic = curl_part(2, d)
    x = (lane // 8).astype(jnp.float32) + x0
    y = (iota((8, 128), 0) + 8 * (group % 2)).astype(jnp.float32) + y0
    z_here = jnp.where(upper, q - 2, q + 126).astype(jnp.float32) + z0
    z_there = z_here + jnp.where(upper, 128.0, -128.0)
    for out, z_at in ((z_out, z_there), (z_fix, z_here)):
        real, imag = contract(frame(x, y, z_at), e, magnetic)
        out[0] = real
        out[1] = imag


def interior_kernel(fields, weights, local, loaded, sem):
    copy = pltpu.make_async_copy(weights, loaded, sem)
    copy.start()
    x0, _ = origin("gx", BLK)
    y0, _ = origin("gy", BLK)
    z0, _ = origin("gz", 128)
    slab = (BLK, 128)
    y = iota(slab, 0).astype(jnp.float32) + y0
    z = iota(slab, 1).astype(jnp.float32) + z0

    def plane(i, carry):
        def at(c, dx=0, dy=0):
            return fields[c, i + (2 + dx), pl.ds(8 + dy, BLK), :]

        def roll(value, by):
            return pltpu.roll(value, by % 128, 1)

        geometry = frame(x0 + i.astype(jnp.float32), y, z)
        k = [at(6 + c) for c in range(6)]
        trace = k[XX] + k[YY] + k[ZZ]
        xx, xy, xz, yy, yz, zz = [value * value for value in k]
        left = xy - zz
        squares = (
            xx - yz + left,
            yy - xz + left,
            k[XY] * (k[XX] + k[YY]) + k[XZ] * k[YZ],
            k[XZ] * (k[XX] + k[ZZ]) + k[XY] * k[YZ],
            k[YZ] * (k[YY] + k[ZZ]) + k[XY] * k[XZ],
        )
        linear = (k[XX] - k[ZZ], k[YY] - k[ZZ], k[XY], k[XZ], k[YZ])
        e = []
        for n, c in enumerate(H_PARTS):
            h = at(c)
            one = (at(c, -1) + at(c, 1)) + (at(c, 0, -1) + at(c, 0, 1)) + (roll(h, 1) + roll(h, -1))
            two = (at(c, -2) + at(c, 2)) + (at(c, 0, -2) + at(c, 0, 2)) + (roll(h, 2) + roll(h, -2))
            e.append(two * FAR - one * (2.0 / 3.0) + h * 3.75 + (trace * linear[n] - squares[n]))

        def slope(m2, m1, p1, p2):
            return (p1 - m1) * NEAR - (p2 - m2) * FAR

        steps = (-2, -1, 1, 2)
        along_x = [pick_k(0, lambda c, s=s: at(c, s)) for s in steps]
        dx = [slope(*[along_x[n][f] for n in range(4)]) for f in range(4)]
        along_y = [pick_k(1, lambda c, s=s: at(c, 0, s)) for s in steps]
        dy = [slope(*[along_y[n][f] for n in range(4)]) for f in range(4)]
        here = [k[YZ], k[XZ], k[XY], k[XX] - k[YY]]
        dz = [slope(*[roll(f, -s) for s in steps]) for f in here]
        parts = [curl_part(axis, d) for axis, d in enumerate((dx, dy, dz))]
        magnetic = [total([part[c] for part in parts]) for c in range(6)]
        real, imag = contract(geometry, e, magnetic)
        local[0, i] = real
        local[1, i] = imag
        return carry

    lax.fori_loop(0, BLK, plane, 0, unroll=2)
    copy.wait()


def transposed_dot(one, two):
    return lax.dot_general(one, two, (((1,), (1,)), ((), ())), preferred_element_type=jnp.float32)


def arrived(place, axis, refs, at):
    even = place % 2 == 0
    one, two = refs[0][at], refs[-1][at]
    before = jnp.where(place > 0, jnp.where(even, two, one), 0.0)
    after = jnp.where(place < lax.axis_size(axis) - 1, jnp.where(even, one, two), 0.0)
    return before, after


def finish_kernel(slots, local, *refs):
    nx, ny, nz = slots
    x_in = refs[:nx]
    y_in = refs[nx : nx + ny]
    z_in = refs[nx + ny : nx + ny + nz]
    z_fix, weights, harm, ids, psi, modes, work, stored, flat, sem = refs[nx + ny + nz :]
    ix = lax.axis_index("gx")
    iy = lax.axis_index("gy")
    iz = lax.axis_index("gz")
    lane = iota((8, 128), 1)
    q = lane % 4
    edge = (lane >= 126) | (lane < 2)
    for part in range(2):
        before, after = arrived(iz, "gz", z_in, part)
        z_part = jnp.where(q < 2, after, before) - z_fix[part]
        for j in range(32):
            moved = pltpu.roll(z_part, (126 - 4 * j) % 128, 1)
            value = local[part, j // 2, pl.ds(8 * (j % 2), 8), :]
            work[part, pl.ds(8 * j, 8), :] = value + jnp.where(edge, moved, 0.0)
    both = work.reshape(512, 128)
    for part in range(2):
        for layer in range(2):
            for place, axis, refs, stride in ((ix, "gx", x_in, 1), (iy, "gy", y_in, BLK)):
                for side, at in zip(arrived(place, axis, refs, (part, layer)), (layer, BLK - 1 - layer)):
                    first = 256 * part + at * (BLK // stride)
                    span = pl.ds(first, BLK, stride=stride) if stride > 1 else pl.ds(first, BLK)
                    both[span, :] = both[span, :] + side
    row = iota((8, 128), 0)
    source = (lane // BLK + row + 1) % 8
    for part in range(2):
        for x in range(BLK):
            rounded = work[part, pl.ds(BLK * x, BLK), :].astype(jnp.bfloat16)
            stored[part, x] = rounded
            values = rounded.astype(jnp.float32)
            for half in range(2):
                value = values[8 * half : 8 * half + 8]
                value = pltpu.roll(value, 0, 1, stride=BLK, stride_axis=0)
                value = jnp.take_along_axis(value, source, axis=0)
                value = pltpu.roll(value, BLK, 1, stride=BLK, stride_axis=0)
                flat[pl.ds(8 * part, 8), pl.ds((2 * x + half) * 128, 128)] = value
    copy = pltpu.make_async_copy(stored, psi, sem)
    copy.start()
    count = ids.shape[1]
    blocks = flat[...].astype(jnp.bfloat16)
    product = transposed_dot(blocks, weights[...])
    own = iota((8, count), 0) == 7 - iota((8, count), 1) // (count // 8)
    real = jnp.sum(jnp.where(own, product[:8], 0.0), axis=0, keepdims=True)
    imag = jnp.sum(jnp.where(own, product[8:], 0.0), axis=0, keepdims=True)
    row = iota((8, count), 0)
    live = ids[...] // PTS == row // 2
    first = row % 2 == 0
    left = jnp.where(live, jnp.where(first, real, imag), 0.0)
    right = jnp.where(live, jnp.where(first, imag, -real), 0.0)
    points = jnp.concatenate([left, right], axis=1)
    main = points.astype(jnp.bfloat16)
    rest = (points - main.astype(jnp.float32)).astype(jnp.bfloat16)
    both = jnp.concatenate([main, rest], axis=0)
    sums = transposed_dot(both, harm[0])
    sums = sums[:8] + sums[8:] + transposed_dot(both, harm[1])[:8]
    sums = sums * (4.0 * math.pi / PTS)
    sums = jnp.concatenate([sums, jnp.zeros((8, 128 - 80), jnp.float32)], axis=1)
    modes[...] = jnp.broadcast_to(sums[None], modes.shape)
    copy.wait()


def swap(value, axis, slot, filler):
    sizes = [lax.axis_size(name) for name in AXES]
    along, aside = AXES.index(axis), AXES.index(filler)
    perm = []
    for place in np.ndindex(*sizes):
        other = list(place)
        other[along] += 1 if place[along] % 2 == slot else -1
        if not 0 <= other[along] < sizes[along]:
            other[along] = place[along]
            other[aside] ^= 1
            if other[aside] >= sizes[aside]:
                continue
        perm.append((int(np.ravel_multi_index(place, sizes)), int(np.ravel_multi_index(other, sizes))))
    return lax.ppermute(value, AXES, perm)


def shards(metric_pert, curvature, interp_weights, point_ids, theta, phi):
    f32 = jnp.float32
    hbm = pl.BlockSpec(memory_space=pltpu.HBM)
    far = lambda value: pltpu.with_memory_space_constraint(value, pltpu.HBM)
    close = lambda value: pltpu.with_memory_space_constraint(value, VMEM)
    vmem = pl.BlockSpec(memory_space=VMEM)
    slots = tuple(min(2, lax.axis_size(axis) - 1) for axis in AXES)
    nx, ny, nz = slots
    count = point_ids.size
    lists = point_ids.shape[2:]
    cells = BLK * BLK * BLK
    face = VMEM((2, 2, BLK, 128), f32)
    edge = VMEM((2, 8, 128), f32)
    params = pltpu.CompilerParams(vmem_limit_bytes=LIMIT)
    bf16 = jnp.bfloat16
    table = VMEM((theta.size // 128, 128), f32)
    first = pl.pallas_call(
        functools.partial(faces_kernel, slots),
        out_shape=[face] * (nx + ny)
        + [edge, edge, VMEM((12, 20, 32, 128), f32), VMEM((2, 80, 2 * count), bf16), VMEM((1, count), jnp.int32)],
        in_specs=[hbm] * 6,
        out_specs=[vmem] * (nx + ny + 5),
        scratch_shapes=[
            VMEM(lists, jnp.int32),
            table,
            table,
            VMEM((ROWS, 128), f32),
            VMEM((80, 2 * count), f32),
            pltpu.SemaphoreType.DMA((6,)),
        ],
        compiler_params=params,
        name="faces",
    )(
        far(metric_pert),
        far(curvature),
        far(point_ids.reshape(lists)),
        far(theta.reshape(-1, 128)),
        far(phi.reshape(-1, 128)),
        far(jnp.asarray(recurrence())),
    )
    x_send, y_send = first[:nx], first[nx : nx + ny]
    z_send, z_fix, fields, harm, ids = first[nx + ny :]
    x_got = [swap(x_send[slot], "gx", slot, "gy") for slot in range(nx)]
    y_got = [swap(y_send[slot], "gy", slot, "gx") for slot in range(ny)]
    z_got = [swap(z_send, "gz", slot, "gy") for slot in range(nz)]
    weights = interp_weights.reshape(count, cells)
    local, loaded = pl.pallas_call(
        interior_kernel,
        out_shape=[VMEM((2, BLK, BLK, 128), f32), VMEM((count, cells), bf16)],
        in_specs=[vmem, hbm],
        out_specs=[vmem] * 2,
        scratch_shapes=[pltpu.SemaphoreType.DMA],
        compiler_params=params,
        cost_estimate=pl.CostEstimate(flops=20_000_000, bytes_accessed=8_000_000, transcendentals=0),
        name="interior",
    )(close(fields), far(weights))
    total_devices = math.prod(lax.axis_size(axis) for axis in AXES)
    psi, modes = pl.pallas_call(
        functools.partial(finish_kernel, slots),
        out_shape=[pltpu.HBM((2, BLK, BLK, 128), jnp.bfloat16), VMEM((total_devices, 8, 128), f32)],
        in_specs=[vmem] * (1 + nx + ny + nz + 4),
        out_specs=[hbm, vmem],
        scratch_shapes=[
            VMEM((2, 256, 128), f32),
            VMEM((2, BLK, BLK, 128), jnp.bfloat16),
            VMEM((16, cells), f32),
            pltpu.SemaphoreType.DMA,
        ],
        compiler_params=params,
        name="finish",
    )(*map(close, (local, *x_got, *y_got, *z_got, z_fix, loaded, harm, ids)))
    modes = lax.all_to_all(modes, AXES, 0, 0, tiled=True).sum(0)
    return psi, modes[: 2 * SPHERES, :MODES].reshape(SPHERES, 2, MODES)


def solution(mesh):
    in_specs = (
        P(None, "gx", "gy", "gz"),
        P(None, "gx", "gy", "gz"),
        P("gx", "gy", "gz", None, None),
        P("gx", "gy", "gz", None),
        P(),
        P(),
    )
    out_specs = (P(None, "gx", "gy", "gz"), P())
    return jax.shard_map(shards, mesh=mesh, in_specs=in_specs, out_specs=out_specs, check_vma=False)
```
